32 devices in a mesh: row: 4 (over y, x), col: 8 (over z, core).
Axes of the slice: x: 2, y: 2, z: 4, core: 2. Of those that a mesh axis runs over, the one named last changes fastest.
Arguments:
- view_one: bfloat16 [2048, 8192], P('row', 'col'), may hold values from -6 to 6
- view_two: bfloat16 [2048, 8192], P('row', 'col'), may hold values from -6 to 6
- pair_weights: bfloat16 [8192, 8192], P('row', 'col'), may hold values from 0.25 to 2.5
Outputs:
- first_grad: bfloat16 [2048, 8192], P('row', 'col')
- second_grad: bfloat16 [2048, 8192], P('row', 'col')
The draws below stay inside these ranges and needn't reach their ends.
All inputs are finite; a program needn't handle non-finite values.
Results may differ from the reference program's by a relative error of at most 0.004.
Values may be sent and summed in bfloat16 or wider, within the bound.
A program may use at most 128 MiB of HBM per device.

```python
import math
import jax
import jax.numpy as jnp

D = 8192
BATCH = 2048


def block_levels(own_key, shape, shards, least, high):
    factor_of, own = 1.0, jax.random.fold_in(own_key, 6)
    for position, shards_of in shards:
        heights = jnp.exp(jax.random.uniform(jax.random.fold_in(own, position), (shards_of,), jnp.float32, least / len(shards), high / len(shards)))
        factor_of = factor_of * jnp.repeat(heights, shape[position] // shards_of).reshape([-1 if axis == position else 1 for axis in range(len(shape))])
    return factor_of


def centred(key, shape, scale, bound, cuts=(), held_as=jnp.bfloat16):
    drawn = scale * jax.random.normal(key, shape, jnp.float32)
    if cuts:
        drawn = drawn * block_levels(key, shape, cuts, -0.22, 0.18)
    return jnp.clip(drawn, -bound, bound).astype(held_as)


def setup_inputs(seed: int = 0) -> dict:
    seeds = jax.random.split(jax.random.key(seed), 4)
    return {
        "view_one": centred(seeds[0], (BATCH, D), 1.0, 6.0, ((0, 4), (1, 8))),
        "view_two": centred(seeds[1], (BATCH, D), 1.0, 6.0, ((0, 4), (1, 8))),
        "pair_weights": jnp.clip(jnp.exp(math.log(2.5) - 2.3025851 * jax.random.uniform(seeds[2], (D, D), jnp.float32) ** block_levels(seeds[2], (D, D), ((0, 4), (1, 8)), -0.2, 0.2)), 0.25, 2.5).astype(jnp.bfloat16),
    }


def reference(view_one, view_two, pair_weights):
    samples = view_one.shape[0]
    correlation = jnp.dot(view_two.T, view_one, preferred_element_type=jnp.float32) / samples
    identity = jnp.eye(D, dtype=jnp.float32)
    weighted = (pair_weights.astype(jnp.float32) * (correlation - identity)).astype(jnp.bfloat16)
    first_grad = jnp.dot(view_two, weighted, preferred_element_type=jnp.float32).astype(jnp.bfloat16)
    second_grad = jnp.dot(view_one, weighted.T, preferred_element_type=jnp.float32).astype(jnp.bfloat16)
    return first_grad, second_grad
```

```python
import jax
import jax.numpy as jnp
from jax import lax
from jax.experimental import pallas as pl
from jax.experimental.pallas import tpu as pltpu
from jax.sharding import PartitionSpec as P

MESH = pl.DeviceIdType.MESH
CORES = 2


def arrived(ref, sem):
    pltpu.make_async_copy(ref, ref, sem).wait()


def gather_kernel(rows, one_ref, two_ref, one_out, two_out, one_held, held, load_sem, up_send, down_send,
                  held_recv, swap_send, swap_recv, one_send, one_recv, pair_send, pair_recv, twin_send, twin_recv):
    samples, width = two_ref.shape
    row, col = lax.axis_index("row"), lax.axis_index("col")
    z, core = lax.div(col, CORES), lax.rem(col, CORES)
    twin = (row, col + 1 - 2 * core)
    core_cols = pl.ds(pl.multiple_of(core * width, width), width)

    def block_rows(index):
        return pl.ds(pl.multiple_of(index * samples, samples), samples)

    def remote(src, dst, send, recv, device):
        return pltpu.make_async_remote_copy(
            src_ref=src, dst_ref=dst, send_sem=send, recv_sem=recv, device_id=device, device_id_type=MESH
        )

    def up(index):
        return remote(held.at[index], held.at[index], up_send.at[index], held_recv.at[index], (row, col + CORES))

    def down(index):
        return remote(held.at[index], held.at[index], down_send.at[index], held_recv.at[index], (row, col - CORES))

    def swap(index):
        return remote(held.at[index], two_out.at[block_rows(row), core_cols], swap_send.at[index],
                      swap_recv.at[row], (index, col))

    def route(index):
        @pl.when(index != row)
        def _():
            swap(index).start()

        @pl.when(index == row)
        def _():
            pltpu.make_async_copy(held.at[index], two_out.at[block_rows(row), core_cols], swap_recv.at[row]).start()

    def one_copy(step):
        target = lax.rem(row + step, rows)
        return remote(one_held, one_out.at[block_rows(row), pl.ds(0, width)], one_send.at[step], one_recv.at[row],
                      (target, col))

    def one_twin(index):
        part = one_out.at[block_rows(index), pl.ds(0, width)]
        return remote(part, one_out.at[block_rows(index), pl.ds(width, width)], pair_send.at[index],
                      pair_recv.at[index], twin)

    def two_twin(index):
        part = two_out.at[block_rows(index), core_cols]
        return remote(part, part, twin_send.at[index], twin_recv.at[index], twin)

    load_two = pltpu.make_async_copy(two_ref, held.at[z], load_sem.at[0])
    load_one = pltpu.make_async_copy(one_ref, one_held, load_sem.at[1])
    load_two.start()
    load_one.start()
    load_two.wait()

    @pl.when(z < rows - 1)
    def _():
        up(z).start()

    @pl.when(z > 0)
    def _():
        down(z).start()

    route(z)
    load_one.wait()
    for step in range(1, rows):
        one_copy(step).start()
    keep_one = pltpu.make_async_copy(one_held, one_out.at[block_rows(row), pl.ds(0, width)], one_recv.at[row])
    keep_one.start()

    for step in range(1, rows):
        @pl.when(z >= step)
        def _(step=step):
            index = z - step
            arrived(held.at[index], held_recv.at[index])

            @pl.when(z < rows - 1)
            def _():
                up(index).start()

            route(index)

        @pl.when(z + step < rows)
        def _(step=step):
            index = z + step
            arrived(held.at[index], held_recv.at[index])

            @pl.when(z > 0)
            def _():
                down(index).start()

            route(index)

    for step in range(rows):
        index = lax.rem(row - step + rows, rows)
        arrived(one_out.at[block_rows(index), pl.ds(0, width)], one_recv.at[index])
        one_twin(index).start()
    for step in range(rows):
        index = lax.rem(row - step + rows, rows)
        arrived(two_out.at[block_rows(index), core_cols], swap_recv.at[index])
        two_twin(index).start()

    twin_cols = pl.ds(pl.multiple_of((1 - core) * width, width), width)
    for index in range(rows):
        one_twin(index).wait_send()
        two_twin(index).wait_send()
        arrived(one_out.at[block_rows(index), pl.ds(width, width)], pair_recv.at[index])
        arrived(two_out.at[block_rows(index), twin_cols], twin_recv.at[index])

        @pl.when(index != row)
        def _(index=index):
            swap(index).wait_send()

        @pl.when(jnp.logical_and(z < rows - 1, index <= z))
        def _(index=index):
            up(index).wait_send()

        @pl.when(jnp.logical_and(z > 0, index >= z))
        def _(index=index):
            down(index).wait_send()
    for step in range(1, rows):
        one_copy(step).wait_send()


def scatter_kernel(rows, first_ref, second_ref, first_out, second_out, parts, moved, terms, first_send, first_recv,
                   move_send, move_recv, term_send, term_recv):
    samples, width = first_out.shape
    row, col = lax.axis_index("row"), lax.axis_index("col")
    z, core = lax.div(col, CORES), lax.rem(col, CORES)

    def block_rows(index):
        return pl.ds(pl.multiple_of(index * samples, samples), samples)

    def remote(src, dst, send, recv, device):
        return pltpu.make_async_remote_copy(
            src_ref=src, dst_ref=dst, send_sem=send, recv_sem=recv, device_id=device, device_id_type=MESH
        )

    def move(step):
        target = lax.rem(row + step, rows)
        return remote(second_ref.at[block_rows(target)], moved.at[row], move_send.at[step], move_recv.at[row],
                      (target, col))

    def first_copy(step):
        target = lax.rem(row + step, rows)
        return remote(first_ref.at[block_rows(target)], parts.at[row], first_send.at[step], first_recv.at[row],
                      (target, col))

    def term(step):
        target = lax.rem(z + step, rows)
        return remote(moved.at[target], terms.at[z], term_send.at[step], term_recv.at[z],
                      (row, target * CORES + core))

    for step in range(1, rows):
        move(step).start()
    pltpu.make_async_copy(second_ref.at[block_rows(row)], moved.at[row], move_recv.at[row]).start()
    for step in range(1, rows):
        first_copy(step).start()
    pltpu.make_async_copy(first_ref.at[block_rows(row)], parts.at[row], first_recv.at[row]).start()
    for step in range(1, rows):
        target = lax.rem(z + step, rows)
        arrived(moved.at[target], move_recv.at[target])
        term(step).start()
    arrived(moved.at[z], move_recv.at[z])
    for index in range(rows):
        arrived(parts.at[index], first_recv.at[index])

    chunk = 64

    def add_first(i, _):
        here = pl.ds(pl.multiple_of(i * chunk, chunk), chunk)
        total = parts[0, here, :].astype(jnp.float32)
        for index in range(1, rows):
            total += parts[index, here, :].astype(jnp.float32)
        first_out[here, :] = total.astype(first_out.dtype)
        return 0

    lax.fori_loop(0, samples // chunk, add_first, 0)
    for step in range(1, rows):
        source = lax.rem(z + step, rows)
        arrived(terms.at[source], term_recv.at[source])

    def add_second(i, _):
        here = pl.ds(pl.multiple_of(i * chunk, chunk), chunk)
        total = moved[z, here, :].astype(jnp.float32)
        for step in range(1, rows):
            total += terms[lax.rem(z + step, rows), here, :].astype(jnp.float32)
        second_out[here, :] = total.astype(second_out.dtype)
        return 0

    lax.fori_loop(0, samples // chunk, add_second, 0)
    for step in range(1, rows):
        move(step).wait_send()
        first_copy(step).wait_send()
        term(step).wait_send()


def gather(rows, view_one, view_two):
    samples, width = view_one.shape
    whole = jax.ShapeDtypeStruct((rows * samples, CORES * width), jnp.bfloat16)
    any_space = pl.BlockSpec(memory_space=pl.ANY)
    dma = pltpu.SemaphoreType.DMA
    return pl.pallas_call(
        lambda *refs: gather_kernel(rows, *refs),
        out_shape=(whole, whole),
        in_specs=[any_space] * 2,
        out_specs=(any_space, any_space),
        scratch_shapes=[
            pltpu.VMEM((samples, width), jnp.bfloat16),
            pltpu.VMEM((rows, samples, width), jnp.bfloat16),
            dma((2,)),
        ] + [dma((rows,))] * 11,
        compiler_params=pltpu.CompilerParams(has_side_effects=True),
        name="gather_views",
    )(view_one, view_two)


def scatter(rows, first, second):
    samples, width = first.shape[0] // rows, first.shape[1]
    own = jax.ShapeDtypeStruct((samples, width), jnp.bfloat16)
    any_space = pl.BlockSpec(memory_space=pl.ANY)
    vmem = pl.BlockSpec(memory_space=pltpu.VMEM)
    blocks = pltpu.VMEM((rows, samples, width), jnp.bfloat16)
    return pl.pallas_call(
        lambda *refs: scatter_kernel(rows, *refs),
        out_shape=(own, own),
        in_specs=[any_space] * 2,
        out_specs=(vmem, vmem),
        scratch_shapes=[blocks, blocks, blocks] + [pltpu.SemaphoreType.DMA((rows,))] * 6,
        compiler_params=pltpu.CompilerParams(has_side_effects=True, vmem_limit_bytes=40 * 2**20),
        name="scatter_grads",
    )(first, second)


def per_device(view_one, view_two, pair_weights):
    rows = lax.axis_size("row")
    samples = view_one.shape[0] * rows
    local_rows, local_cols = pair_weights.shape
    row, col = lax.axis_index("row"), lax.axis_index("col")
    core = lax.rem(col, CORES)
    one_pair, two_rows = gather(rows, view_one, view_two)
    summed = lax.dot_general(
        two_rows, one_pair[:, :local_cols], (((0,), (0,)), ((), ())), preferred_element_type=jnp.float32
    )
    row_ids = row * local_rows + lax.broadcasted_iota(jnp.int32, (local_rows, local_cols), 0)
    col_ids = col * local_cols + lax.broadcasted_iota(jnp.int32, (local_rows, local_cols), 1)
    identity = jnp.where(row_ids == col_ids, 1.0, 0.0).astype(jnp.float32)
    weighted = (pair_weights.astype(jnp.float32) * (summed / samples - identity)).astype(jnp.bfloat16)
    mine = lax.dynamic_slice_in_dim(weighted, core * local_cols, local_cols, 0)
    other = lax.dynamic_slice_in_dim(weighted, (1 - core) * local_cols, local_cols, 0)
    pairs = [(i, i + 1 - 2 * (i % CORES)) for i in range(lax.axis_size("col"))]
    theirs = lax.ppermute(other, "col", pairs)
    first = jnp.dot(two_rows, weighted, preferred_element_type=jnp.float32).astype(jnp.bfloat16)
    across = jnp.concatenate([mine, theirs], axis=1)
    second = lax.dot_general(
        one_pair, across, (((1,), (1,)), ((), ())), preferred_element_type=jnp.float32
    ).astype(jnp.bfloat16)
    return scatter(rows, first, second)


def solution(mesh):
    placed = (P("row", "col"), P("row", "col"), P("row", "col"))
    return jax.shard_map(
        per_device,
        mesh=mesh,
        in_specs=placed,
        out_specs=(P("row", "col"), P("row", "col")),
        check_vma=False,
    )
```

```python
import jax
import jax.numpy as jnp
from jax import lax
from jax.experimental import pallas as pl
from jax.experimental.pallas import tpu as pltpu
from jax.sharding import PartitionSpec as P

MESH = pl.DeviceIdType.MESH
CORES = 2
PIECES = 4


def arrived(ref, sem):
    pltpu.make_async_copy(ref, ref, sem).wait()


def remote(src, dst, send, recv, device):
    return pltpu.make_async_remote_copy(
        src_ref=src, dst_ref=dst, send_sem=send, recv_sem=recv, device_id=device, device_id_type=MESH
    )


def gather_kernel(rows, one_ref, two_ref, one_out, two_out, one_held, held, load_sem, one_send, one_recv, pair_send,
                  pair_recv, up_send, down_send, held_recv, swap_send, swap_recv, twin_send, twin_recv):
    samples, width = two_ref.shape
    piece = samples // PIECES
    row, col = lax.axis_index("row"), lax.axis_index("col")
    z, core = lax.div(col, CORES), lax.rem(col, CORES)
    twin = (row, col + 1 - 2 * core)
    core_cols = pl.ds(pl.multiple_of(core * width, width), width)
    twin_cols = pl.ds(pl.multiple_of((1 - core) * width, width), width)

    def block_rows(index):
        return pl.ds(pl.multiple_of(index * samples, samples), samples)

    def piece_rows(index, q):
        return pl.ds(pl.multiple_of(index * samples + q * piece, piece), piece)

    def held_piece(index, q):
        return held.at[index, pl.ds(q * piece, piece)]

    def up(index, q):
        part = held_piece(index, q)
        return remote(part, part, up_send.at[index, q], held_recv.at[index, q], (row, col + CORES))

    def down(index, q):
        part = held_piece(index, q)
        return remote(part, part, down_send.at[index, q], held_recv.at[index, q], (row, col - CORES))

    def swap(index, q):
        return remote(held_piece(index, q), two_out.at[piece_rows(row, q), core_cols], swap_send.at[index, q],
                      swap_recv.at[row, q], (index, col))

    def route(index, q):
        @pl.when(index != row)
        def _():
            swap(index, q).start()

        @pl.when(index == row)
        def _():
            pltpu.make_async_copy(held_piece(index, q), two_out.at[piece_rows(row, q), core_cols],
                                  swap_recv.at[row, q]).start()

    def one_copy(step):
        target = lax.rem(row + step, rows)
        return remote(one_held, one_out.at[block_rows(row), pl.ds(0, width)], one_send.at[step], one_recv.at[row],
                      (target, col))

    def one_twin(index):
        part = one_out.at[block_rows(index), pl.ds(0, width)]
        return remote(part, one_out.at[block_rows(index), pl.ds(width, width)], pair_send.at[index],
                      pair_recv.at[index], twin)

    def two_twin(index, q):
        part = two_out.at[piece_rows(index, q), core_cols]
        return remote(part, part, twin_send.at[index, q], twin_recv.at[index, q], twin)

    def pass_up(index, q):
        @pl.when(z < rows - 1)
        def _():
            up(index, q).start()

    def pass_down(index, q):
        @pl.when(z > 0)
        def _():
            down(index, q).start()

    def own(q):
        pass_up(z, q)
        pass_down(z, q)
        route(z, q)

    load_two = pltpu.make_async_copy(two_ref, held.at[z], load_sem.at[0])
    load_one = pltpu.make_async_copy(one_ref, one_held, load_sem.at[1])
    load_two.start()
    load_one.start()
    load_two.wait()
    own(0)
    load_one.wait()
    for step in range(1, rows):
        one_copy(step).start()
    pltpu.make_async_copy(one_held, one_out.at[block_rows(row), pl.ds(0, width)], one_recv.at[row]).start()

    for q in range(PIECES):
        if q + 1 < PIECES:
            own(q + 1)
        for step in range(1, rows):
            @pl.when(z >= step)
            def _(step=step, q=q):
                arrived(held_piece(z - step, q), held_recv.at[z - step, q])
                pass_up(z - step, q)
                route(z - step, q)

            @pl.when(z + step < rows)
            def _(step=step, q=q):
                arrived(held_piece(z + step, q), held_recv.at[z + step, q])
                pass_down(z + step, q)
                route(z + step, q)

    for step in range(rows):
        index = lax.rem(row - step + rows, rows)
        arrived(one_out.at[block_rows(index), pl.ds(0, width)], one_recv.at[index])
        one_twin(index).start()
    for q in range(PIECES):
        for step in range(rows):
            index = lax.rem(row - step + rows, rows)
            arrived(two_out.at[piece_rows(index, q), core_cols], swap_recv.at[index, q])
            two_twin(index, q).start()

    for index in range(rows):
        one_twin(index).wait_send()
        arrived(one_out.at[block_rows(index), pl.ds(width, width)], pair_recv.at[index])
        for q in range(PIECES):
            two_twin(index, q).wait_send()
            arrived(two_out.at[piece_rows(index, q), twin_cols], twin_recv.at[index, q])

            @pl.when(index != row)
            def _(index=index, q=q):
                swap(index, q).wait_send()

            @pl.when(jnp.logical_and(z < rows - 1, index <= z))
            def _(index=index, q=q):
                up(index, q).wait_send()

            @pl.when(jnp.logical_and(z > 0, index >= z))
            def _(index=index, q=q):
                down(index, q).wait_send()
    for step in range(1, rows):
        one_copy(step).wait_send()


def scatter_kernel(rows, one_ref, two_ref, weighted_ref, first_out, second_out, one_held, two_held, weighted, theirs,
                   first_sent, parts, second_sent, moved, from_below, from_above, load_sem, twin_sem, first_send,
                   first_recv, move_send, move_recv, up_send, up_recv, down_send, down_recv):
    samples, width = first_out.shape
    tile = width // PIECES
    row, col = lax.axis_index("row"), lax.axis_index("col")
    z, core = lax.div(col, CORES), lax.rem(col, CORES)

    def half(which):
        return pl.ds(pl.multiple_of(which * width, width), width)

    def move(target, q):
        return remote(second_sent.at[q, target], moved.at[q, row], move_send.at[q, target], move_recv.at[q, row],
                      (target, col))

    def first_copy(target, q):
        return remote(first_sent.at[q, target], parts.at[q, row], first_send.at[q, target], first_recv.at[q, row],
                      (target, col))

    def up(index, q):
        return remote(moved.at[q, index], from_below.at[q, index], up_send.at[q, index], up_recv.at[q, index],
                      (row, col + CORES))

    def down(index, q):
        return remote(moved.at[q, index], from_above.at[q, index], down_send.at[q, index], down_recv.at[q, index],
                      (row, col - CORES))

    def first_tile(target, q):
        cols = pl.ds(pl.multiple_of(q * tile, tile), tile)
        mine = two_held[pl.ds(pl.multiple_of(target * samples, samples), samples), :]
        return jnp.dot(mine, weighted[:, cols], preferred_element_type=jnp.float32).astype(jnp.bfloat16)

    def second_tile(target, q):
        here = pl.ds(pl.multiple_of(target * samples, samples), samples)
        contract = (((1,), (1,)), ((), ()))
        near = weighted[pl.ds(pl.multiple_of(core * width + q * tile, tile), tile), :]
        far = theirs[pl.ds(pl.multiple_of(q * tile, tile), tile), :]
        total = lax.dot_general(one_held[here, pl.ds(0, width)], near, contract, preferred_element_type=jnp.float32)
        total += lax.dot_general(one_held[here, pl.ds(width, width)], far, contract,
                                 preferred_element_type=jnp.float32)
        return total.astype(jnp.bfloat16)

    exchange = remote(weighted_ref.at[half(1 - core)], theirs, twin_sem.at[0], twin_sem.at[1],
                      (row, col + 1 - 2 * core))
    exchange.start()
    loads = [pltpu.make_async_copy(src, dst, load_sem.at[i]) for i, (src, dst) in enumerate(
        ((weighted_ref, weighted), (two_ref, two_held), (one_ref, one_held)))]
    for load in loads:
        load.start()
    loads[0].wait()
    loads[1].wait()

    def own_first(q, _):
        parts[q, row] = first_tile(row, q)
        return 0

    lax.fori_loop(0, PIECES, own_first, 0)
    loads[2].wait()
    exchange.wait()

    def seconds(i, _):
        q, step = lax.div(i, rows), lax.rem(i, rows) + 1
        target = lax.rem(row + step, rows)
        value = second_tile(target, q)

        @pl.when(target == row)
        def _():
            moved[q, row] = value

        @pl.when(target != row)
        def _():
            second_sent[q, target] = value
            move(target, q).start()

        return 0

    lax.fori_loop(0, PIECES * rows, seconds, 0)

    def firsts(i, _):
        q, step = lax.div(i, rows - 1), lax.rem(i, rows - 1) + 1
        target = lax.rem(row + step, rows)
        first_sent[q, target] = first_tile(target, q)
        first_copy(target, q).start()
        return 0

    lax.fori_loop(0, PIECES * (rows - 1), firsts, 0)

    def settle(index, q):
        @pl.when(index != row)
        def _():
            arrived(moved.at[q, index], move_recv.at[q, index])

    def chain(i, _):
        q, turn = lax.div(i, rows - 1), lax.rem(i, rows - 1)
        above = rows - 1 - (turn - z)
        below = turn - (rows - 1 - z)

        @pl.when(jnp.logical_and(turn >= z, above > z))
        def _():
            settle(above, q)

            @pl.when(z > 0)
            def _():
                arrived(from_below.at[q, above], up_recv.at[q, above])
                moved[q, above] = (moved[q, above].astype(jnp.float32)
                                   + from_below[q, above].astype(jnp.float32)).astype(jnp.bfloat16)

            up(above, q).start()

        @pl.when(jnp.logical_and(below >= 0, below < z))
        def _():
            settle(below, q)

            @pl.when(z < rows - 1)
            def _():
                arrived(from_above.at[q, below], down_recv.at[q, below])
                moved[q, below] = (moved[q, below].astype(jnp.float32)
                                   + from_above[q, below].astype(jnp.float32)).astype(jnp.bfloat16)

            down(below, q).start()

        return 0

    lax.fori_loop(0, PIECES * (rows - 1), chain, 0)

    for q in range(PIECES):
        cols = pl.ds(q * tile, tile)
        for step in range(1, rows):
            index = lax.rem(row + step, rows)
            arrived(parts.at[q, index], first_recv.at[q, index])
        total = parts[q, 0].astype(jnp.float32)
        for index in range(1, rows):
            total += parts[q, index].astype(jnp.float32)
        first_out[:, cols] = total.astype(first_out.dtype)
    for q in range(PIECES):
        cols = pl.ds(q * tile, tile)
        settle(z, q)

        @pl.when(z > 0)
        def _(q=q):
            arrived(from_below.at[q, z], up_recv.at[q, z])

        @pl.when(z < rows - 1)
        def _(q=q):
            arrived(from_above.at[q, z], down_recv.at[q, z])

        @pl.when(z == 0)
        def _(q=q, cols=cols):
            second_out[:, cols] = (moved[q, z].astype(jnp.float32)
                                   + from_above[q, z].astype(jnp.float32)).astype(second_out.dtype)

        @pl.when(z == rows - 1)
        def _(q=q, cols=cols):
            second_out[:, cols] = (moved[q, z].astype(jnp.float32)
                                   + from_below[q, z].astype(jnp.float32)).astype(second_out.dtype)

        @pl.when(jnp.logical_and(z > 0, z < rows - 1))
        def _(q=q, cols=cols):
            second_out[:, cols] = (moved[q, z].astype(jnp.float32) + from_below[q, z].astype(jnp.float32)
                                   + from_above[q, z].astype(jnp.float32)).astype(second_out.dtype)

    for q in range(PIECES):
        for step in range(1, rows):
            target = lax.rem(row + step, rows)
            move(target, q).wait_send()
            first_copy(target, q).wait_send()
        for index in range(rows):
            @pl.when(index > z)
            def _(index=index, q=q):
                up(index, q).wait_send()

            @pl.when(index < z)
            def _(index=index, q=q):
                down(index, q).wait_send()


def gather(rows, view_one, view_two):
    samples, width = view_one.shape
    whole = jax.ShapeDtypeStruct((rows * samples, CORES * width), jnp.bfloat16)
    any_space = pl.BlockSpec(memory_space=pl.ANY)
    dma = pltpu.SemaphoreType.DMA
    return pl.pallas_call(
        lambda *refs: gather_kernel(rows, *refs),
        out_shape=(whole, whole),
        in_specs=[any_space] * 2,
        out_specs=(any_space, any_space),
        scratch_shapes=[
            pltpu.VMEM((samples, width), jnp.bfloat16),
            pltpu.VMEM((rows, samples, width), jnp.bfloat16),
            dma((2,)),
        ] + [dma((rows,))] * 4 + [dma((rows, PIECES))] * 7,
        compiler_params=pltpu.CompilerParams(has_side_effects=True),
        name="gather_views",
    )(view_one, view_two)


def scatter(rows, one_pair, two_rows, weighted):
    height, width = weighted.shape
    samples = one_pair.shape[0] // rows
    own = jax.ShapeDtypeStruct((samples, width), jnp.bfloat16)
    any_space = pl.BlockSpec(memory_space=pl.ANY)
    vmem = pl.BlockSpec(memory_space=pltpu.VMEM)
    blocks = pltpu.VMEM((PIECES, rows, samples, width // PIECES), jnp.bfloat16)
    views = pltpu.VMEM(one_pair.shape, jnp.bfloat16)
    dma = pltpu.SemaphoreType.DMA
    return pl.pallas_call(
        lambda *refs: scatter_kernel(rows, *refs),
        out_shape=(own, own),
        in_specs=[any_space] * 3,
        out_specs=(vmem, vmem),
        scratch_shapes=[
            views,
            views,
            pltpu.VMEM((height, width), jnp.bfloat16),
            pltpu.VMEM((width, width), jnp.bfloat16),
        ] + [blocks] * 6 + [dma((3,)), dma((2,))] + [dma((PIECES, rows))] * 8,
        compiler_params=pltpu.CompilerParams(has_side_effects=True, vmem_limit_bytes=60 * 2**20),
        name="scatter_grads",
    )(one_pair, two_rows, weighted)


def per_device(view_one, view_two, pair_weights):
    rows = lax.axis_size("row")
    samples = view_one.shape[0] * rows
    local_rows, local_cols = pair_weights.shape
    row, col = lax.axis_index("row"), lax.axis_index("col")
    one_pair, two_rows = gather(rows, view_one, view_two)
    summed = lax.dot_general(
        two_rows, one_pair[:, :local_cols], (((0,), (0,)), ((), ())), preferred_element_type=jnp.float32
    )
    row_ids = row * local_rows + lax.broadcasted_iota(jnp.int32, (local_rows, local_cols), 0)
    col_ids = col * local_cols + lax.broadcasted_iota(jnp.int32, (local_rows, local_cols), 1)
    identity = jnp.where(row_ids == col_ids, 1.0, 0.0).astype(jnp.float32)
    weighted = (pair_weights.astype(jnp.float32) * (summed / samples - identity)).astype(jnp.bfloat16)
    return scatter(rows, one_pair, two_rows, weighted)


def solution(mesh):
    placed = (P("row", "col"), P("row", "col"), P("row", "col"))
    return jax.shard_map(
        per_device,
        mesh=mesh,
        in_specs=placed,
        out_specs=(P("row", "col"), P("row", "col")),
        check_vma=False,
    )
```
